768 devices in a mesh: dp: 192 (over y, z, core), sp: 4 (over x).
Axes of the slice: x: 4, y: 8, z: 12, core: 2. Of those that a mesh axis runs over, the one named last changes fastest.
Arguments:
- hidden: bfloat16 [192, 4, 128, 3584], P('dp', None, 'sp'), may hold values from -6 to 6
- segment_ids: int32 [192, 4, 128], P('dp'), may hold values from -1 to 15, as said below
- w_query: bfloat16 [3584, 3584], P(None, 'sp'), may hold values from -0.10022297 to 0.10022297
- key_matrix: bfloat16 [3584, 512], P(None, 'sp'), may hold values from -0.10022297 to 0.10022297
- value_matrix: bfloat16 [3584, 512], P(None, 'sp'), may hold values from -0.10022297 to 0.10022297
Outputs:
- mixed: bfloat16 [192, 512, 3584], P('dp', 'sp')
The draws below stay inside these ranges and needn't reach their ends.
Inputs may be any that keep to these rules, and one draw needn't show every extreme that they name: `segment_ids`: in each outbox the live slots come first; over them the ids start at 0 and never fall, by steps of 0 or 1; empty slots hold -1. Every group has an outbox whose 128 slots are all live.
All inputs are finite; a program needn't handle non-finite values.
Results may differ from the reference program's by a relative error of at most 0.0087.
Values may be sent and summed in bfloat16 or wider, within the bound.
A program may use at most 64 MiB of HBM per device.

```python
import math
import jax
import jax.numpy as jnp
from jax import lax

MODEL_WIDTH = 3584
QUERY_HEADS = 28
KEY_VALUE_HEADS = 4
HEAD_SIZE = 128
J = 4
B = 128
NSEG = 16
NG = 192
GROUP_SLOTS = 512


def drawn_parts(key):
    key_dir = jax.random.fold_in(key, 21)
    single_key_head = jax.random.fold_in(key, 22)
    direction = jnp.clip(jax.random.normal(key_dir, (MODEL_WIDTH,), jnp.float32), -4.0, 4.0)
    direction = direction / jnp.sqrt(jnp.sum(direction * direction))
    mask_pattern = jnp.clip(jax.random.normal(single_key_head, (KEY_VALUE_HEADS, HEAD_SIZE), jnp.float32), -4.0, 4.0)
    return (direction, mask_pattern)


def draw_w_query(key, part):
    direction, mask_pattern = drawn_parts(key)
    random_noise_key = jax.random.fold_in(key, 31)
    initial_sample = jnp.clip(jax.random.normal(random_noise_key, (MODEL_WIDTH, QUERY_HEADS * HEAD_SIZE), jnp.float32), -5.0, 5.0)
    split_by_head = jnp.repeat(mask_pattern, QUERY_HEADS // KEY_VALUE_HEADS, axis=0).reshape(QUERY_HEADS * HEAD_SIZE)
    weight = initial_sample / math.sqrt(MODEL_WIDTH) + HEAD_SIZE ** (-0.25) * direction[:, None] * split_by_head[None, :]
    bound_value = 6.0 / math.sqrt(MODEL_WIDTH)
    return jnp.clip(weight, -bound_value, bound_value).astype(jnp.bfloat16)


def draw_key_matrix(key, part):
    direction, mask_pattern = drawn_parts(key)
    random_noise_key = jax.random.fold_in(key, 32)
    initial_sample = jnp.clip(jax.random.normal(random_noise_key, (MODEL_WIDTH, KEY_VALUE_HEADS * HEAD_SIZE), jnp.float32), -5.0, 5.0)
    split_by_head = mask_pattern.reshape(KEY_VALUE_HEADS * HEAD_SIZE)
    weight = initial_sample / math.sqrt(MODEL_WIDTH) + HEAD_SIZE ** (-0.25) * direction[:, None] * split_by_head[None, :]
    bound_value = 6.0 / math.sqrt(MODEL_WIDTH)
    return jnp.clip(weight, -bound_value, bound_value).astype(jnp.bfloat16)


def draw_value_matrix(key, part):
    direction = drawn_parts(key)[0]
    random_noise_key = jax.random.fold_in(key, 33)
    initial_sample = jnp.clip(jax.random.normal(random_noise_key, (MODEL_WIDTH, KEY_VALUE_HEADS * HEAD_SIZE), jnp.float32), -5.0, 5.0)
    initial_sample = initial_sample / math.sqrt(MODEL_WIDTH)
    along = jnp.sum(direction[:, None] * initial_sample, axis=0)
    weight = initial_sample - direction[:, None] * along[None, :]
    bound_value = 6.0 / math.sqrt(MODEL_WIDTH)
    return jnp.clip(weight, -bound_value, bound_value).astype(jnp.bfloat16)


def draw_hidden(key, part):
    direction = drawn_parts(key)[0]
    random_noise_key = jax.random.fold_in(key, 41)
    start_key = jax.random.fold_in(key, 42)
    level_key = jax.random.fold_in(key, 43)
    noise_draw = jnp.clip(jax.random.normal(random_noise_key, (NG, J, B, MODEL_WIDTH), jnp.float32), -5.0, 5.0)
    strengths = jnp.array([110.0, 160.0, 220.0, 300.0], jnp.float32)
    run_length = max(B // 8, 2)
    starts = jax.random.randint(start_key, (NG, J), 0, B // 4 - run_length + 1)
    levels = jax.random.randint(level_key, (NG, J), 0, 4)
    picked = (levels[..., None] == jnp.arange(4, dtype=jnp.int32)).astype(jnp.float32)
    amplitude = jnp.sqrt(jnp.sum(picked * strengths, axis=-1))
    slot_index = jnp.arange(B, dtype=jnp.int32)
    inside = (slot_index[None, None, :] >= starts[..., None]) & (slot_index[None, None, :] < starts[..., None] + run_length)
    boost_size = jnp.where(inside, amplitude[..., None], 0.0)
    mixed_rows = noise_draw + boost_size[..., None] * direction
    return jnp.clip(mixed_rows, -6.0, 6.0).astype(jnp.bfloat16)


def draw_segment_ids(key, part):
    key_live = jax.random.fold_in(key, 11)
    key_full = jax.random.fold_in(key, 12)
    key_cuts = jax.random.fold_in(key, 13)
    live_count = jax.random.randint(key_live, (NG, J), B // 4, B + 1)
    full_box = jax.random.randint(key_full, (NG,), 0, J)
    live_count = jnp.where(jnp.arange(J)[None, :] == full_box[:, None], B, live_count)
    index = jnp.arange(B, dtype=jnp.int32)
    cut_marks = (jax.random.randint(key_cuts, (NG, J, B), 0, 12) == 0) & (index[None, None, :] > 0)
    seg_ids = jnp.minimum(jnp.cumsum(cut_marks.astype(jnp.int32), axis=-1), NSEG - 1)
    return jnp.where(index[None, None, :] < live_count[:, :, None], seg_ids, -1).astype(jnp.int32)


def setup_inputs(seed: int = 0) -> dict:
    splits = jax.random.split(jax.random.key(seed), 6)
    hidden = draw_hidden(jax.random.fold_in(splits[5], 71), 0)
    segment_ids = draw_segment_ids(jax.random.fold_in(splits[5], 71), 0)
    w_query = draw_w_query(jax.random.fold_in(splits[5], 71), 0)
    key_matrix = draw_key_matrix(jax.random.fold_in(splits[5], 71), 0)
    value_matrix = draw_value_matrix(jax.random.fold_in(splits[5], 71), 0)
    return dict(hidden=hidden, segment_ids=segment_ids, w_query=w_query, key_matrix=key_matrix, value_matrix=value_matrix)


ROPE_BASE = 1000000.0

def rotate(tensor, where):
    half_width = tensor.shape[-1] // 2
    freq = ROPE_BASE ** (-(jnp.arange(half_width, dtype=jnp.float32) * 2.0 / tensor.shape[-1]))
    angle = where[:, None] * freq[None, :]
    cosine = jnp.cos(angle)[:, None, :]
    sine = jnp.sin(angle)[:, None, :]
    first = tensor[..., :half_width]
    second = tensor[..., half_width:]
    return jnp.concatenate([first * cosine - second * sine, second * cosine + first * sine], axis=-1)

def positions(segments):
    slot_ids = jnp.arange(NSEG, dtype=jnp.int32)
    onehot = (segments[..., :, None] == slot_ids).astype(jnp.int32)
    living = (segments >= 0).astype(jnp.int32)
    below = lax.optimization_barrier(jnp.sum((segments[..., :, None] < slot_ids).astype(jnp.int32) * living[..., :, None], axis=-2))
    first_slot = lax.optimization_barrier(jnp.sum(onehot * below[..., None, :], axis=-1))
    index = jnp.arange(segments.shape[-1], dtype=jnp.int32)
    return (index - first_slot).astype(jnp.float32)

def attend(queries, projected_key_rows, projected_value_rows, labels):
    total_rows = queries.shape[0]
    kv_heads = projected_key_rows.shape[1]
    queries = queries.reshape(total_rows, kv_heads, -1, queries.shape[-1]).astype(jnp.float32)
    scores = jnp.einsum('qcgd,kcd->cgqk', queries, projected_key_rows.astype(jnp.float32)) / jnp.sqrt(jnp.float32(queries.shape[-1]))
    index = jnp.arange(total_rows, dtype=jnp.int32)
    seen = (labels[:, None] == labels[None, :]) & (labels[:, None] >= 0) & (index[None, :] <= index[:, None])
    seen = seen | (index[:, None] == index[None, :])
    scores = jnp.where(seen, scores, -1e+30)
    largest = lax.optimization_barrier(jnp.max(scores, axis=-1, keepdims=True))
    expo = jnp.where(seen, jnp.exp(scores - largest), 0.0)
    denominator = lax.optimization_barrier(jnp.sum(expo, axis=-1, keepdims=True))
    probs = expo.astype(jnp.bfloat16).astype(jnp.float32)
    summed = jnp.einsum('cgqk,kcd->qcgd', probs, projected_value_rows.astype(jnp.float32))
    summed = summed / jnp.transpose(denominator, (2, 0, 1, 3))
    living = (labels >= 0).astype(jnp.float32)
    return (summed.reshape(total_rows, -1) * living[:, None]).astype(jnp.bfloat16)

def reference(hidden, segment_ids, w_query, key_matrix, value_matrix):
    received = jnp.stack([jnp.roll(hidden[:, outbox], outbox, axis=0) for outbox in range(J)], axis=1)
    segments = jnp.stack([jnp.roll(segment_ids[:, outbox], outbox, axis=0) for outbox in range(J)], axis=1)
    where_all = positions(segments)
    box_ids = jnp.arange(J, dtype=jnp.int32)[None, :, None]
    labels = jnp.where(segments >= 0, box_ids * NSEG + segments, -1)

    def one_group(packed):
        slab, where, label_row = packed
        flattened_slots = slab.reshape(GROUP_SLOTS, MODEL_WIDTH)
        where = where.reshape(GROUP_SLOTS)
        queries = jnp.dot(flattened_slots, w_query, preferred_element_type=jnp.float32).reshape(GROUP_SLOTS, QUERY_HEADS, HEAD_SIZE)
        queries = rotate(queries, where).astype(jnp.bfloat16)
        projected_key_rows = jnp.dot(flattened_slots, key_matrix, preferred_element_type=jnp.float32).reshape(GROUP_SLOTS, KEY_VALUE_HEADS, HEAD_SIZE)
        projected_key_rows = rotate(projected_key_rows, where).astype(jnp.bfloat16)
        projected_value_rows = jnp.dot(flattened_slots, value_matrix, preferred_element_type=jnp.float32).astype(jnp.bfloat16).reshape(GROUP_SLOTS, KEY_VALUE_HEADS, HEAD_SIZE)
        return attend(queries, projected_key_rows, projected_value_rows, label_row.reshape(GROUP_SLOTS))
    return lax.map(one_group, (received, where_all, labels))
```

```python
import functools
import math

import jax
import jax.numpy as jnp
from jax import lax
from jax.experimental import pallas as pl
from jax.experimental.pallas import tpu as pltpu
from jax.sharding import PartitionSpec as P

HEAD = 128
BOXES = 4
ROPE_BASE = 1000000.0
MESH = pl.DeviceIdType.MESH


def kernel(hidden, seg, w_query, key_matrix, value_matrix, freq, out,
           tok, segs, weights, cosine, sine, seen, alive, queries, keys, values, staged, relay,
           load_sem, shift_send, shift_recv, seg_send, seg_recv,
           own_send, own_recv, pass_send, pass_recv,
           give_send, give_recv, hop_send, hop_recv, end_send, end_recv):
    ndp = lax.axis_size("dp")
    nsp = lax.axis_size("sp")
    me_dp = lax.axis_index("dp")
    me = lax.axis_index("sp")
    core = lax.rem(me_dp, 2)
    right = lax.rem(me + 1, nsp)
    left = lax.rem(me + nsp - 1, nsp)
    across = lax.rem(me + 2, nsp)
    part = hidden.shape[2]
    half = part // 2
    rows = BOXES * part
    q_cols = w_query.shape[1]
    heads = q_cols // HEAD

    def box_of(step):
        return lax.select(core == 0, step, lax.rem(BOXES - step, BOXES))

    def slot(box, owner):
        return tok.at[box, pl.ds(pl.multiple_of(owner * part, part), part)]

    def slot_half(box, owner, which):
        return tok.at[box, pl.ds(pl.multiple_of(owner * part + which * half, half), half)]

    def remote(src, dst, send, recv, dp, sp):
        return pltpu.make_async_remote_copy(
            src_ref=src, dst_ref=dst, send_sem=send, recv_sem=recv,
            device_id=(dp, sp), device_id_type=MESH)

    loads = [
        pltpu.make_async_copy(hidden.at[0, 0], slot(0, me), load_sem.at[0]),
        pltpu.make_async_copy(seg.at[0], segs.at[0], load_sem.at[1]),
        pltpu.make_async_copy(key_matrix, weights.at[:, pl.ds(q_cols, HEAD)], load_sem.at[2]),
        pltpu.make_async_copy(value_matrix, weights.at[:, pl.ds(q_cols + HEAD, HEAD)], load_sem.at[3]),
        pltpu.make_async_copy(w_query, weights.at[:, pl.ds(0, q_cols)], load_sem.at[4]),
    ]
    for load in loads:
        load.start()

    barrier = pltpu.get_barrier_semaphore()
    for step in (1, 2, 3):
        pl.semaphore_signal(barrier, inc=1, device_id=(lax.rem(me_dp + step, ndp), me), device_id_type=MESH)
        pl.semaphore_signal(barrier, inc=1, device_id=(lax.rem(me_dp + ndp - step, ndp), me), device_id_type=MESH)
    for peer in (right, left, across):
        pl.semaphore_signal(barrier, inc=1, device_id=(me_dp, peer), device_id_type=MESH)
    pl.semaphore_wait(barrier, 9)

    def own_copy(src, box, direction, which):
        peer = right if direction == 0 else left
        return remote(src, slot_half(box, me, which), own_send.at[box, direction, which],
                      own_recv.at[box, direction, which], me_dp, peer)

    def own_start(box, source):
        for order in (0, 1):
            for direction in (0, 1):
                which = order if direction == 0 else 1 - order
                own_copy(source(which), box, direction, which).start()

    def pass_copy(box, direction):
        peer = right if direction == 0 else left
        origin = left if direction == 0 else right
        return remote(slot_half(box, origin, direction), slot_half(box, origin, direction),
                      pass_send.at[box, direction], pass_recv.at[box, direction], me_dp, peer)

    def own_wait(box, direction, which):
        origin = left if direction == 0 else right
        remote(slot_half(box, origin, which), slot_half(box, origin, which),
               own_send.at[box, direction, which], own_recv.at[box, direction, which],
               me_dp, right).wait_recv()

    def seg_copy(box):
        return remote(seg.at[0], segs.at[box], seg_send.at[box], seg_recv.at[box],
                      lax.rem(me_dp + box, ndp), me)

    def shift_copy(box):
        return remote(hidden.at[0, box], slot(box, me), shift_send.at[box], shift_recv.at[box],
                      lax.rem(me_dp + box, ndp), me)

    own_start(0, lambda which: hidden.at[0, 0, pl.ds(which * half, half)])
    for box in (1, 2, 3):
        seg_copy(box).start()
    for order in (1, 2, 3):
        shift_copy(lax.select(core == 0, BOXES - order, order)).start()

    def give_columns(origin):
        return pl.ds(pl.multiple_of(origin * q_cols, HEAD), q_cols)

    def give_right(box):
        return remote(staged.at[box], out.at[0, :, give_columns(me)], give_send.at[0],
                      give_recv.at[0], me_dp, right)

    def give_left(box):
        return remote(staged.at[box], out.at[0, :, give_columns(me)], give_send.at[1],
                      give_recv.at[1], me_dp, left)

    def hop(box, direction):
        peer = right if direction == 0 else left
        return remote(staged.at[box, pl.ds(direction * (rows // 2), rows // 2)], relay.at[direction],
                      hop_send.at[direction], hop_recv.at[direction], me_dp, peer)

    def end_hop(direction):
        peer = right if direction == 0 else left
        origin = left if direction == 0 else right
        return remote(relay.at[direction],
                      out.at[0, pl.ds(direction * (rows // 2), rows // 2), give_columns(origin)],
                      end_send.at[direction], end_recv.at[direction], me_dp, peer)

    def keep(box):
        return pltpu.make_async_copy(staged.at[box], out.at[0, :, give_columns(me)], load_sem.at[5])

    def give(box):
        delta = lax.rem(box + nsp - me, nsp)

        @pl.when(delta == 0)
        def _():
            keep(box).start()

        @pl.when(delta == 1)
        def _():
            give_right(box).start()

        @pl.when(delta == 3)
        def _():
            give_left(box).start()

        @pl.when(delta == 2)
        def _():
            hop(box, 0).start()
            hop(box, 1).start()

    scale = 1.0 / math.sqrt(HEAD)
    row_id = lax.broadcasted_iota(jnp.int32, (rows, rows), 0)
    col_id = lax.broadcasted_iota(jnp.int32, (rows, rows), 1)

    def body(step, carry):
        box = box_of(step)
        for direction in (0, 1):
            own_wait(box, direction, direction)
            pass_copy(box, direction).start()

        @pl.when(step < BOXES - 1)
        def _():
            later = box_of(step + 1)
            shift_copy(later).wait_recv()
            own_start(later, lambda which: slot_half(later, me, which))

        @pl.when(step == BOXES - 1)
        def _():
            for before in range(BOXES - 1):
                give(box_of(before))

        @pl.when(step == 0)
        def _():
            loads[1].wait()

        @pl.when(step > 0)
        def _():
            seg_copy(box).wait_recv()

        seg_row = jnp.broadcast_to(segs[box, pl.ds(box, 1), :], (rows, rows))
        seg_col = jnp.transpose(seg_row)
        below = jnp.where((seg_row >= 0) & (seg_row < seg_col), 1.0, 0.0)
        first = jnp.sum(below, axis=1, keepdims=True)
        where = row_id.astype(jnp.float32) - first
        angle = where * freq[0:1, :]
        cosine[...] = jnp.cos(angle)
        swing = jnp.sin(angle)
        sine[...] = jnp.where(col_id < HEAD // 2, -swing, swing)
        same = (seg_row == seg_col) & (seg_col >= 0) & (col_id <= row_id)
        seen[...] = jnp.where(same | (col_id == row_id), 0.0, -1e30)
        alive[...] = jnp.where(seg_col >= 0, 1.0, 0.0)

        @pl.when(step == 0)
        def _():
            for load in (loads[0], loads[2], loads[3], loads[4]):
                load.wait()

        for direction in (0, 1):
            own_wait(box, direction, 1 - direction)
            pass_copy_wait = remote(
                slot_half(box, across, direction), slot_half(box, across, direction),
                pass_send.at[box, direction], pass_recv.at[box, direction], me_dp, right)
            pass_copy_wait.wait_recv()

        def turned(value):
            return value * cosine[...] + pltpu.roll(value, HEAD // 2, 1) * sine[...]

        both = jnp.dot(tok[box], weights[:, q_cols:], preferred_element_type=jnp.float32)
        keys[...] = turned(both[:, :HEAD]).astype(jnp.bfloat16)
        values[...] = both[:, HEAD:].astype(jnp.bfloat16)
        for begin in range(0, heads, 2):
            count = min(2, heads - begin)
            product = jnp.dot(tok[box], weights[:, begin * HEAD:(begin + count) * HEAD],
                              preferred_element_type=jnp.float32)
            for index in range(count):
                query = turned(product[:, index * HEAD:(index + 1) * HEAD])
                queries[begin + index] = query.astype(jnp.bfloat16)
        for index in range(heads):
            scores = lax.dot_general(queries[index], keys[...], (((1,), (1,)), ((), ())),
                                     preferred_element_type=jnp.float32) * scale
            scores = jnp.where(seen[...] == 0.0, scores, -1e30)
            top = jnp.max(scores, axis=1, keepdims=True)
            expo = jnp.exp(scores - top)
            total = jnp.sum(expo, axis=1, keepdims=True)
            mixed = jnp.dot(expo.astype(jnp.bfloat16), values[...], preferred_element_type=jnp.float32)
            mixed = mixed * (alive[...] / total)
            staged[box, :, index * HEAD:(index + 1) * HEAD] = mixed.astype(jnp.bfloat16)

        @pl.when(step == BOXES - 1)
        def _():
            give(box)
        return carry

    lax.fori_loop(0, BOXES, body, 0)

    for direction in (0, 1):
        hop(0, direction).wait_recv()
        end_hop(direction).start()
    give_right(0).wait()
    give_left(0).wait()
    keep(0).wait()
    for direction in (0, 1):
        hop(0, direction).wait_send()
        end_hop(direction).wait()
    for box in (1, 2, 3):
        seg_copy(box).wait_send()
        shift_copy(box).wait_send()
    for box in range(BOXES):
        for direction in (0, 1):
            pass_copy(box, direction).wait_send()
            for which in (0, 1):
                own_copy(slot_half(box, me, which), box, direction, which).wait_send()


def local(hidden, segment_ids, w_query, key_matrix, value_matrix):
    depth = hidden.shape[3]
    part = hidden.shape[2]
    rows = BOXES * part
    q_cols = w_query.shape[1]
    width = q_cols + 2 * HEAD
    heads = q_cols // HEAD
    freq = ROPE_BASE ** (-(jnp.arange(HEAD // 2, dtype=jnp.float32) * 2.0 / HEAD))
    freq = jnp.broadcast_to(jnp.concatenate([freq, freq])[None, :], (8, HEAD))
    dma = pltpu.SemaphoreType.DMA
    flops = 2 * BOXES * rows * depth * width
    return pl.pallas_call(
        kernel,
        out_shape=jax.ShapeDtypeStruct((1, rows, 4 * q_cols), jnp.bfloat16),
        in_specs=[pl.BlockSpec(memory_space=pltpu.HBM)] * 5 + [pl.BlockSpec(memory_space=pltpu.VMEM)],
        out_specs=pl.BlockSpec(memory_space=pltpu.HBM),
        scratch_shapes=[
            pltpu.VMEM((BOXES, rows, depth), jnp.bfloat16),
            pltpu.VMEM((BOXES, BOXES, rows), jnp.int32),
            pltpu.VMEM((depth, width), jnp.bfloat16),
            pltpu.VMEM((rows, HEAD), jnp.float32),
            pltpu.VMEM((rows, HEAD), jnp.float32),
            pltpu.VMEM((rows, rows), jnp.float32),
            pltpu.VMEM((rows, HEAD), jnp.float32),
            pltpu.VMEM((heads, rows, HEAD), jnp.bfloat16),
            pltpu.VMEM((rows, HEAD), jnp.bfloat16),
            pltpu.VMEM((rows, HEAD), jnp.bfloat16),
            pltpu.VMEM((BOXES, rows, q_cols), jnp.bfloat16),
            pltpu.VMEM((2, rows // 2, q_cols), jnp.bfloat16),
            dma((6,)),
            dma((BOXES,)), dma((BOXES,)),
            dma((BOXES,)), dma((BOXES,)),
            dma((BOXES, 2, 2)), dma((BOXES, 2, 2)),
            dma((BOXES, 2)), dma((BOXES, 2)),
            dma((2,)), dma((2,)),
            dma((2,)), dma((2,)),
            dma((2,)), dma((2,)),
        ],
        compiler_params=pltpu.CompilerParams(
            collective_id=0, has_side_effects=True, vmem_limit_bytes=40 * 1024 * 1024),
        cost_estimate=pl.CostEstimate(flops=flops, bytes_accessed=12000000, transcendentals=0),
        name="fused_boxes",
    )(hidden, segment_ids, w_query, key_matrix, value_matrix, freq)


def solution(mesh):
    placed = (
        P("dp", None, "sp", None),
        P("dp", None, None),
        P(None, "sp"),
        P(None, "sp"),
        P(None, "sp"),
    )
    return jax.shard_map(
        local, mesh=mesh, in_specs=placed, out_specs=P("dp", "sp", None), check_vma=False
    )
```

```python
import functools
import math

import jax
import jax.numpy as jnp
from jax import lax
from jax.experimental import pallas as pl
from jax.experimental.pallas import tpu as pltpu
from jax.sharding import PartitionSpec as P

HEAD = 128
BOXES = 4
ROPE_BASE = 1000000.0
Z_CHIPS = 12
VMEM_LIMIT = 55300000
MESH = pl.DeviceIdType.MESH


def kernel(hidden, seg, w_query, key_matrix, value_matrix, out,
           tok, segs, weights, cosine, sine, seen, alive, queries, keys, values, staged, mine,
           load_sem, shift_send, shift_recv, seg_send, seg_recv,
           own_send, own_recv, pass_send, pass_recv, give_send, give_recv):
    ndp = lax.axis_size("dp")
    nsp = lax.axis_size("sp")
    me_dp = lax.axis_index("dp")
    me = lax.axis_index("sp")
    core = lax.rem(me_dp, 2)
    first_plane = lax.rem(lax.div(me_dp, 2), Z_CHIPS) == 0
    right = lax.rem(me + 1, nsp)
    left = lax.rem(me + nsp - 1, nsp)
    across = lax.rem(me + 2, nsp)
    part = hidden.shape[2]
    half = part // 2
    rows = BOXES * part
    q_cols = w_query.shape[1]
    heads = q_cols // HEAD

    def box_of(step):
        return lax.select((core == 1) & (step >= 2), 5 - step, step)

    def slot(box, owner):
        return tok.at[box, pl.ds(pl.multiple_of(owner * part, part), part)]

    def slot_half(box, owner, which):
        return tok.at[box, pl.ds(pl.multiple_of(owner * part + which * half, half), half)]

    def remote(src, dst, send, recv, dp, sp):
        return pltpu.make_async_remote_copy(
            src_ref=src, dst_ref=dst, send_sem=send, recv_sem=recv,
            device_id=(dp, sp), device_id_type=MESH)

    barrier = pltpu.get_barrier_semaphore()
    for peer in (right, left, across):
        pl.semaphore_signal(barrier, inc=1, device_id=(me_dp, peer), device_id_type=MESH)
    for box in (1, 2, 3):
        pl.semaphore_signal(barrier, inc=1, device_id=(lax.rem(me_dp + ndp - box, ndp), me), device_id_type=MESH)

    loads = [
        pltpu.make_async_copy(hidden.at[0, 0], slot(0, me), load_sem.at[0]),
        pltpu.make_async_copy(hidden.at[0, pl.ds(1, BOXES - 1)], mine, load_sem.at[1]),
        pltpu.make_async_copy(seg.at[0], segs.at[0], load_sem.at[5]),
        pltpu.make_async_copy(key_matrix, weights.at[:, pl.ds(q_cols, HEAD)], load_sem.at[2]),
        pltpu.make_async_copy(value_matrix, weights.at[:, pl.ds(q_cols + HEAD, HEAD)], load_sem.at[3]),
        pltpu.make_async_copy(w_query, weights.at[:, pl.ds(0, q_cols)], load_sem.at[4]),
    ]
    for load in loads:
        load.start()
    pl.semaphore_wait(barrier, 6)
    loads[0].wait()
    loads[1].wait()

    def own_copy(box, direction, which):
        peer = right if direction == 0 else left
        return remote(slot_half(box, me, which), slot_half(box, me, which), own_send.at[box, direction, which],
                      own_recv.at[box, direction, which], me_dp, peer)

    def own_start(box):
        for order in (0, 1):
            for direction in (0, 1):
                which = order if direction == 0 else 1 - order
                own_copy(box, direction, which).start()

    def pass_copy(box, direction):
        peer = right if direction == 0 else left
        origin = left if direction == 0 else right
        return remote(slot_half(box, origin, direction), slot_half(box, origin, direction),
                      pass_send.at[box, direction], pass_recv.at[box, direction], me_dp, peer)

    def own_wait(box, direction, which):
        origin = left if direction == 0 else right
        remote(slot_half(box, origin, which), slot_half(box, origin, which),
               own_send.at[box, direction, which], own_recv.at[box, direction, which],
               me_dp, right).wait_recv()

    def pass_wait(box, direction):
        remote(slot_half(box, across, direction), slot_half(box, across, direction),
               pass_send.at[box, direction], pass_recv.at[box, direction], me_dp, right).wait_recv()

    def seg_copy(box):
        return remote(segs.at[0], segs.at[box], seg_send.at[box], seg_recv.at[box],
                      lax.rem(me_dp + box, ndp), me)

    def shift_copy(box):
        return remote(mine.at[box - 1], slot(box, me), shift_send.at[box], shift_recv.at[box],
                      lax.rem(me_dp + box, ndp), me)

    def spread(step):
        shift_copy(box_of(step)).wait_recv()
        own_start(box_of(step))

    def forward(step):
        for direction in (0, 1):
            own_wait(box_of(step), direction, direction)
            pass_copy(box_of(step), direction).start()

    own_start(0)
    shift_copy(1).start()
    loads[2].wait()
    for box in (1, 2, 3):
        seg_copy(box).start()
    for box in (2, 3):
        shift_copy(box).start()
    forward(0)

    @pl.when(jnp.logical_not(first_plane & (core == 0)))
    def _():
        spread(1)

    def give_columns(origin):
        return pl.ds(pl.multiple_of(origin * q_cols, HEAD), q_cols)

    def give_copy(box, origin, delta):
        return remote(staged.at[box], out.at[0, :, give_columns(origin)], give_send.at[delta],
                      give_recv.at[origin], me_dp, box)

    def keep(box):
        return pltpu.make_async_copy(staged.at[box], out.at[0, :, give_columns(me)], load_sem.at[6])

    def give(box):
        delta = lax.rem(box + nsp - me, nsp)

        @pl.when(delta == 0)
        def _():
            keep(box).start()

        @pl.when(delta != 0)
        def _():
            give_copy(box, me, delta).start()

    scale = 1.0 / math.sqrt(HEAD)
    row_id = lax.broadcasted_iota(jnp.int32, (rows, rows), 0)
    col_id = lax.broadcasted_iota(jnp.int32, (rows, rows), 1)

    def body(step, carry):
        box = box_of(step)
        held = first_plane & (step == core)

        @pl.when((step < BOXES - 1) & jnp.logical_not(held))
        def _():
            forward(step + 1)

        @pl.when((step < BOXES - 2) & jnp.logical_not(first_plane & (step <= core)))
        def _():
            spread(step + 2)

        @pl.when(step > 0)
        def _():
            seg_copy(box).wait_recv()

        seg_row = jnp.broadcast_to(segs[box, pl.ds(box, 1), :], (rows, rows))
        seg_col = jnp.transpose(seg_row)
        below = jnp.where((seg_row >= 0) & (seg_row < seg_col), 1.0, 0.0)
        first = jnp.sum(below, axis=1, keepdims=True)
        where = row_id.astype(jnp.float32) - first
        lane = lax.rem(col_id, HEAD // 2).astype(jnp.float32)
        freq = jnp.exp(lane * (-2.0 * math.log(ROPE_BASE) / HEAD))
        angle = where * freq
        cosine[...] = jnp.cos(angle)
        swing = jnp.sin(angle)
        sine[...] = jnp.where(col_id < HEAD // 2, -swing, swing)
        same = (seg_row == seg_col) & (seg_col >= 0) & (col_id <= row_id)
        seen[...] = jnp.where(same | (col_id == row_id), 0.0, -1e30)
        alive[...] = jnp.where(seg_col >= 0, 1.0, 0.0)

        @pl.when(step == 0)
        def _():
            for load in loads[3:]:
                load.wait()

        for direction in (0, 1):
            own_wait(box, direction, 1 - direction)
            pass_wait(box, direction)

        @pl.when(step == BOXES - 1)
        def _():
            give(box_of(2))
            give(box_of(1))

            @pl.when(jnp.logical_not(first_plane & (core == 0)))
            def _():
                give(box_of(0))

        def turned(value):
            return value * cosine[...] + pltpu.roll(value, HEAD // 2, 1) * sine[...]

        both = jnp.dot(tok[box], weights[:, q_cols:], preferred_element_type=jnp.float32)
        keys[...] = turned(both[:, :HEAD]).astype(jnp.bfloat16)
        values[...] = both[:, HEAD:].astype(jnp.bfloat16)
        for begin in range(0, heads, 2):
            count = min(2, heads - begin)
            product = jnp.dot(tok[box], weights[:, begin * HEAD:(begin + count) * HEAD],
                              preferred_element_type=jnp.float32)
            for index in range(count):
                query = turned(product[:, index * HEAD:(index + 1) * HEAD])
                queries[begin + index] = query.astype(jnp.bfloat16)
        for index in range(heads):
            scores = lax.dot_general(queries[index], keys[...], (((1,), (1,)), ((), ())),
                                     preferred_element_type=jnp.float32) * scale
            scores = jnp.where(seen[...] == 0.0, scores, -1e30)
            top = jnp.max(scores, axis=1, keepdims=True)
            expo = jnp.exp(scores - top)
            total = jnp.sum(expo, axis=1, keepdims=True)
            mixed = jnp.dot(expo.astype(jnp.bfloat16), values[...], preferred_element_type=jnp.float32)
            mixed = mixed * (alive[...] / total)
            staged[box, :, index * HEAD:(index + 1) * HEAD] = mixed.astype(jnp.bfloat16)

        @pl.when((step == BOXES - 1) | (first_plane & (core == 0) & (step == 0)))
        def _():
            give(box)

        @pl.when(held)
        def _():
            spread(step + 1)
            forward(step + 1)
            spread(step + 2)
        return carry

    lax.fori_loop(0, BOXES, body, 0)

    for delta in (1, 2, 3):
        give_copy(0, lax.rem(me + delta, nsp), delta).wait_recv()
        give_copy(0, me, delta).wait_send()
    keep(0).wait()
    for box in (1, 2, 3):
        seg_copy(box).wait_send()
        shift_copy(box).wait_send()
    for box in range(BOXES):
        for direction in (0, 1):
            pass_copy(box, direction).wait_send()
            for which in (0, 1):
                own_copy(box, direction, which).wait_send()


def local(hidden, segment_ids, w_query, key_matrix, value_matrix):
    depth = hidden.shape[3]
    part = hidden.shape[2]
    rows = BOXES * part
    q_cols = w_query.shape[1]
    width = q_cols + 2 * HEAD
    heads = q_cols // HEAD
    dma = pltpu.SemaphoreType.DMA
    flops = 2 * BOXES * rows * depth * width
    return pl.pallas_call(
        kernel,
        out_shape=jax.ShapeDtypeStruct((1, rows, 4 * q_cols), jnp.bfloat16),
        in_specs=[pl.BlockSpec(memory_space=pltpu.HBM)] * 5,
        out_specs=pl.BlockSpec(memory_space=pltpu.HBM),
        scratch_shapes=[
            pltpu.VMEM((BOXES, rows, depth), jnp.bfloat16),
            pltpu.VMEM((BOXES, BOXES, rows), jnp.int32),
            pltpu.VMEM((depth, width), jnp.bfloat16),
            pltpu.VMEM((rows, HEAD), jnp.float32),
            pltpu.VMEM((rows, HEAD), jnp.float32),
            pltpu.VMEM((rows, rows), jnp.float32),
            pltpu.VMEM((rows, HEAD), jnp.float32),
            pltpu.VMEM((heads, rows, HEAD), jnp.bfloat16),
            pltpu.VMEM((rows, HEAD), jnp.bfloat16),
            pltpu.VMEM((rows, HEAD), jnp.bfloat16),
            pltpu.VMEM((BOXES, rows, q_cols), jnp.bfloat16),
            pltpu.VMEM((BOXES - 1, part, depth), jnp.bfloat16),
            dma((7,)),
            dma((BOXES,)), dma((BOXES,)),
            dma((BOXES,)), dma((BOXES,)),
            dma((BOXES, 2, 2)), dma((BOXES, 2, 2)),
            dma((BOXES, 2)), dma((BOXES, 2)),
            dma((BOXES,)), dma((BOXES,)),
        ],
        compiler_params=pltpu.CompilerParams(
            collective_id=0, has_side_effects=True, vmem_limit_bytes=VMEM_LIMIT),
        cost_estimate=pl.CostEstimate(flops=flops, bytes_accessed=12000000, transcendentals=0),
        name="fused_boxes",
    )(hidden, segment_ids, w_query, key_matrix, value_matrix)


def solution(mesh):
    placed = (
        P("dp", None, "sp", None),
        P("dp", None, None),
        P(None, "sp"),
        P(None, "sp"),
        P(None, "sp"),
    )
    return jax.shard_map(
        local, mesh=mesh, in_specs=placed, out_specs=P("dp", "sp", None), check_vma=False
    )
```
